32 devices in a mesh: seq: 16 (over z, y, x), tp: 2 (over core).
Axes of the slice: x: 2, y: 2, z: 4, core: 2. Of those that a mesh axis runs over, the one named last changes fastest.
Arguments:
- img_qkv: bfloat16 [1, 512, 3, 2048], P(None, 'seq', None, 'tp'), may hold values from -7 to 7
- txt_qkv: bfloat16 [1, 256, 3, 2048], P(None, None, None, 'tp'), may hold values from -7 to 7
- frame_index: int32 [1, 512], P(None, 'seq'), may hold values from 0 to 32
- row_index: int32 [1, 512], P(None, 'seq'), may hold values from 0 to 44
- column_index: int32 [1, 512], P(None, 'seq'), may hold values from 0 to 79
- txt_len: int32 [1], replicated, may hold values from 64 to 256
- residual: bfloat16 [1, 512, 3072], P(None, ('seq', 'tp')), may hold values from -6 to 6
- w_proj: bfloat16 [2048, 3072], P('tp'), may hold values from -0.125 to 0.125
- proj_bias: float32 [3072], replicated, may hold values from -3 to 3
- gate: float32 [3072], replicated, may hold values from -4 to 4
Outputs:
- img_out: bfloat16 [1, 512, 3072], P(None, ('seq', 'tp'))
- txt_out: bfloat16 [1, 256, 2048], P(None, None, 'tp')
The draws below stay inside these ranges and needn't reach their ends.
All inputs are finite; a program needn't handle non-finite values.
Results may differ from the reference program's by a relative error of at most 0.0082.
Values may be sent and summed in bfloat16 or wider, within the bound.
A program may use at most 64 MiB of HBM per device.

```python
import math
import jax
import jax.numpy as jnp
from jax import lax

D = 3072
HD = 128
HEADS = 16
TXT = 256
LAT_T = 33
LAT_H = 45
LAT_W = 80
CLIPS = 1
IMG = 512
QW = 2048


def draw_img_qkv(key, part):
    width_all = HEADS * HD
    total_rows = CLIPS * IMG
    subkeys = jax.random.split(jax.random.fold_in(key, 11), 4)
    query_part = jnp.clip(1.8 * jax.random.normal(subkeys[0], (total_rows, width_all), jnp.float32), -7.0, 7.0)
    key_part = jnp.clip(1.8 * jax.random.normal(subkeys[1], (total_rows, width_all), jnp.float32), -7.0, 7.0)
    value_part = jnp.clip(jax.random.normal(subkeys[3], (total_rows, width_all), jnp.float32), -6.0, 6.0)
    stacked = jnp.stack([query_part, key_part, value_part], axis=1)
    return stacked.reshape(CLIPS, IMG, 3, width_all).astype(jnp.bfloat16)


def draw_txt_qkv(key, part):
    width_all = HEADS * HD
    subkeys = jax.random.split(jax.random.fold_in(key, 23), 4)
    query_part = jnp.clip(1.8 * jax.random.normal(subkeys[0], (CLIPS, TXT, width_all), jnp.float32), -7.0, 7.0)
    key_part = jnp.clip(1.8 * jax.random.normal(subkeys[1], (CLIPS, TXT, width_all), jnp.float32), -7.0, 7.0)
    value_part = jnp.clip(jax.random.normal(subkeys[3], (CLIPS, TXT, width_all), jnp.float32), -6.0, 6.0)
    return jnp.stack([query_part, key_part, value_part], axis=2).astype(jnp.bfloat16)


def plant(values, own_key, low, high):
    extent = values.shape
    index_at = [jax.random.randint(jax.random.fold_in(own_key, axis), (), 0, extent[axis]) for axis in range(len(extent))]
    values = values.at[tuple(index_at)].set(low)
    longest = extent.index(max(extent))
    index_at[longest] = (index_at[longest] + 1) % extent[longest]
    return values.at[tuple(index_at)].set(high)


def steps_of(key, dims, cuts, least, high):
    def one(dim, parts):
        steps = jax.random.uniform(jax.random.fold_in(jax.random.fold_in(key, 6), dim), (parts,), jnp.float32, least / len(cuts), high / len(cuts))
        return jnp.repeat(jnp.exp(steps), dims[dim] // parts).reshape((-1,) + (1,) * (len(dims) - dim - 1))

    factor_of = one(*cuts[0])
    for cut in cuts[1:]:
        factor_of = factor_of * one(*cut)
    return factor_of


def normal_values(rng, shape, scale, limit, cuts=(), held_as=jnp.bfloat16):
    values = scale * jax.random.normal(rng, shape, jnp.float32)
    if cuts:
        values = values * steps_of(rng, shape, cuts, -0.22, 0.18)
    return jnp.clip(values, -limit, limit).astype(held_as)


def setup_inputs(seed: int = 0) -> dict:
    seeds = jax.random.split(jax.random.key(seed), 11)
    img_qkv = draw_img_qkv(jax.random.fold_in(seeds[10], 71), 0)
    txt_qkv = draw_txt_qkv(jax.random.fold_in(seeds[10], 71), 0)
    frame_index = plant(jax.random.randint(seeds[2], (CLIPS, IMG), 0, LAT_T), jax.random.fold_in(seeds[2], 1), 0, LAT_T - 1).astype(jnp.int32)
    row_index = plant(jax.random.randint(seeds[3], (CLIPS, IMG), 0, LAT_H), jax.random.fold_in(seeds[3], 1), 0, LAT_H - 1).astype(jnp.int32)
    column_index = plant(jax.random.randint(seeds[4], (CLIPS, IMG), 0, LAT_W), jax.random.fold_in(seeds[4], 1), 0, LAT_W - 1).astype(jnp.int32)
    txt_len = jax.random.randint(seeds[5], (CLIPS,), TXT // 4, TXT + 1).astype(jnp.int32)
    residual = normal_values(seeds[6], (CLIPS, IMG, D), 1.0, 6.0, ((1, 32),))
    w_proj = normal_values(seeds[7], (QW, D), QW ** -0.5, 0.125, ((0, 2),))
    proj_bias = normal_values(seeds[8], (D,), 0.5, 3.0, (), jnp.float32)
    gate = normal_values(seeds[9], (D,), 1.0, 4.0, (), jnp.float32)
    return {"img_qkv": img_qkv, "txt_qkv": txt_qkv, "frame_index": frame_index, "row_index": row_index, "column_index": column_index, "txt_len": txt_len, "residual": residual, "w_proj": w_proj, "proj_bias": proj_bias, "gate": gate}


rope_base = 256.0
neg_large = -1e+30

def rope_tables(frame_index, row_index, column_index, head_dim):
    frame_part = head_dim // 8
    second = (head_dim - frame_part) // 2
    pieces = []
    for places, part_width in ((frame_index, frame_part), (row_index, second), (column_index, second)):
        pair_ids = jnp.arange(part_width // 2).astype(jnp.float32)
        pair_rates = rope_base ** (-2.0 * pair_ids / part_width)
        pieces.append(places.astype(jnp.float32)[:, None] * pair_rates[None, :])
    angles = jnp.repeat(jnp.concatenate(pieces, axis=1), 2, axis=1)
    parity = jnp.arange(head_dim) % 2
    signed = jnp.where(parity == 0, -1.0, 1.0).astype(jnp.float32)
    return (jnp.cos(angles), jnp.sin(angles) * signed[None, :])

def rotate(block_in, cosine, sine_table):
    values = block_in.astype(jnp.float32)
    parity = jnp.arange(values.shape[-1]) % 2
    partner = jnp.where(parity == 0, jnp.roll(values, -1, axis=-1), jnp.roll(values, 1, axis=-1))
    return (values * cosine[:, None, :] + partner * sine_table[:, None, :]).astype(jnp.bfloat16)

def attend_head(query_head, key_head, value_head, live_keys):
    row_count = query_head.shape[0]
    row_block = 1
    for candidate in range(1, 1025):
        if row_count % candidate == 0:
            row_block = candidate
    blocks = query_head.reshape(row_count // row_block, row_block, query_head.shape[1])
    score_scale = 1.0 / math.sqrt(query_head.shape[1])

    def one_block(query_block):
        scores = jnp.dot(query_block, key_head.T, preferred_element_type=jnp.float32) * score_scale
        scores = jnp.where(live_keys[None, :], scores, neg_large)
        peak = lax.optimization_barrier(jnp.max(scores, axis=1, keepdims=True))
        weights = jnp.where(live_keys[None, :], jnp.exp(scores - peak), 0.0)
        weight_sum = lax.optimization_barrier(jnp.sum(weights, axis=1, keepdims=True))
        blended = jnp.dot(weights.astype(jnp.bfloat16), value_head, preferred_element_type=jnp.float32)
        return (blended / weight_sum).astype(jnp.bfloat16)
    return lax.map(one_block, blocks).reshape(row_count, query_head.shape[1])

def clip_attention(clip_qkv, clip_txt, frames, rows_at, columns_at, length):
    cosine, sine_table = rope_tables(frames, rows_at, columns_at, HD)
    img_query = rotate(clip_qkv[:, 0].reshape(IMG, HEADS, HD), cosine, sine_table)
    img_key = rotate(clip_qkv[:, 1].reshape(IMG, HEADS, HD), cosine, sine_table)
    img_value = clip_qkv[:, 2].reshape(IMG, HEADS, HD)
    queries = jnp.concatenate([img_query, clip_txt[:, 0].reshape(TXT, HEADS, HD)], axis=0)
    all_keys = jnp.concatenate([img_key, clip_txt[:, 1].reshape(TXT, HEADS, HD)], axis=0)
    all_values = jnp.concatenate([img_value, clip_txt[:, 2].reshape(TXT, HEADS, HD)], axis=0)
    live_keys = jnp.arange(IMG + TXT) < IMG + length

    def head_work(operands):
        return attend_head(operands[0], operands[1], operands[2], live_keys)
    attended = lax.map(head_work, (queries.transpose(1, 0, 2), all_keys.transpose(1, 0, 2), all_values.transpose(1, 0, 2)))
    joined = attended.transpose(1, 0, 2).reshape(IMG + TXT, HEADS * HD)
    img_rows = joined[:IMG]
    txt_rows = joined[IMG:]
    txt_live = jnp.arange(TXT) < length
    txt_rows = jnp.where(txt_live[:, None], txt_rows, jnp.zeros_like(txt_rows))
    return (img_rows, txt_rows)

def reference(img_qkv, txt_qkv, frame_index, row_index, column_index, txt_len, residual, w_proj, proj_bias, gate):
    img_outs = []
    txt_outs = []
    for clip in range(CLIPS):
        img_rows, txt_rows = clip_attention(img_qkv[clip], txt_qkv[clip], frame_index[clip], row_index[clip], column_index[clip], txt_len[clip])
        projected = jnp.dot(img_rows, w_proj, preferred_element_type=jnp.float32)
        mixed = residual[clip].astype(jnp.float32) + gate[None, :] * (projected + proj_bias[None, :])
        img_outs.append(mixed.astype(jnp.bfloat16))
        txt_outs.append(txt_rows)
    return (jnp.stack(img_outs, axis=0), jnp.stack(txt_outs, axis=0))
```

```python
import functools
import math

import jax
import jax.numpy as jnp
import numpy as np
from jax import lax
from jax.experimental import pallas as pl
from jax.experimental.pallas import tpu as pltpu
from jax.sharding import PartitionSpec as P

HD = 128
ROPE_BASE = 256.0
NEG_LARGE = -1e30
F32 = jnp.float32
BF16 = jnp.bfloat16


def pair_rates():
    first = HD // 8
    second = (HD - first) // 2
    rates = np.zeros((3, HD), np.float32)
    start = 0
    for part, width in enumerate((first, second, second)):
        ids = np.arange(width // 2, dtype=np.float64)
        rates[part, start : start + width] = np.repeat(ROPE_BASE ** (-2.0 * ids / width), 2)
        start += width
    return rates


def largest_divisor(n):
    best = 1
    for d in range(1, n + 1):
        if n % d == 0 and d * d <= n:
            best = d
    return best


def kernel(
    n, heads, img_ref, txt_ref, pos_ref, rates_ref, len_ref, res_hbm, w_hbm, bias_hbm, gate_hbm,
    out_ref, txt_out,
    q_send, k_send, q_all, k_all, v_all, a_send, home, t_send, w, res, bias, gate, p_send, p_recv,
    local_sem, q_ss, q_rs, k_ss, k_rs, v_ss, v_rs, a_ss, a_rs, t1_ss, t2_ss, t_rs, p_ss, p_rs,
):
    p = lax.axis_index("seq")
    t = lax.axis_index("tp")
    groups = n // heads
    head = p // groups
    group = p % groups
    tokens = img_ref.shape[1]
    text = txt_ref.shape[1]
    share = text // groups
    image_keys = n * tokens
    scale = 1.0 / math.sqrt(HD)
    chunks = p_send.shape[0]
    width = p_send.shape[2]
    half = tokens // 2
    plane = largest_divisor(n)
    lines = n // plane

    loads = [
        pltpu.make_async_copy(src, dst, local_sem.at[i])
        for i, (src, dst) in enumerate(
            ((w_hbm, w), (res_hbm, res), (bias_hbm, bias), (gate_hbm, gate))
        )
    ]
    for load in loads:
        load.start()

    barrier = pltpu.get_barrier_semaphore()

    def greet(o, carry):
        pl.semaphore_signal(barrier, inc=1, device_id={"seq": (p + o) % n})
        return carry

    lax.fori_loop(1, n, greet, 0)
    pl.semaphore_signal(barrier, inc=1, device_id={"tp": 1 - t})

    diagonal = lax.broadcasted_iota(jnp.int32, (tokens, tokens), 0) == lax.broadcasted_iota(
        jnp.int32, (tokens, tokens), 1
    )
    angles = jnp.zeros((tokens, HD), F32)
    for part in range(3):
        row = pos_ref[part : part + 1, :].astype(F32)
        column = jnp.sum(jnp.where(diagonal, row, 0.0), axis=1, keepdims=True)
        angles = angles + column * rates_ref[part : part + 1, :]
    even = lax.broadcasted_iota(jnp.int32, (tokens, HD), 1) % 2 == 0
    cosine = jnp.cos(angles)
    sine = jnp.where(even, -1.0, 1.0) * jnp.sin(angles)
    for which, dst in ((0, q_send), (1, k_send)):
        for h in range(heads):
            x = img_ref[which, :, h * HD : (h + 1) * HD].astype(F32)
            partner = jnp.where(even, pltpu.roll(x, HD - 1, 1), pltpu.roll(x, 1, 1))
            dst[h] = (x * cosine + partner * sine).astype(BF16)

    pl.semaphore_wait(barrier, n)

    def rows(s):
        return pl.ds(pl.multiple_of(s * tokens, tokens), tokens)

    def cols(h):
        return pl.ds(pl.multiple_of(h * HD, HD), HD)

    def q_copy(h, src_line):
        return pltpu.make_async_remote_copy(
            q_send.at[h], q_all.at[rows(src_line)], q_ss.at[h], q_rs.at[src_line],
            device_id={"seq": h * groups + group},
        )

    def k_copy(d, s):
        return pltpu.make_async_remote_copy(
            k_send.at[d // groups], k_all.at[rows(s)], k_ss.at[d], k_rs.at[s], device_id={"seq": d}
        )

    def v_copy(d, s):
        return pltpu.make_async_remote_copy(
            img_ref.at[2, :, cols(d // groups)], v_all.at[rows(s)], v_ss.at[d], v_rs.at[s],
            device_id={"seq": d},
        )

    def a_copy(j, h):
        return pltpu.make_async_remote_copy(
            a_send.at[rows(j)], home.at[:, cols(h)], a_ss.at[j], a_rs.at[h],
            device_id={"seq": j * groups + group},
        )

    def over(count, f):
        def step(o, carry):
            f(o)
            return carry

        lax.fori_loop(1, count, step, 0)

    over(n, lambda o: k_copy((p + o) % n, p).start())
    over(heads, lambda o: q_copy((head + o) % heads, head).start())
    over(n, lambda o: v_copy((p + o) % n, p).start())

    q_all[rows(head), :] = q_send[head]
    k_all[rows(p), :] = k_send[head]
    v_all[rows(p), :] = img_ref[2, :, cols(head)]
    k_all[image_keys : image_keys + text, :] = txt_ref[1]
    v_all[image_keys : image_keys + text, :] = txt_ref[2]
    length = len_ref[0]

    def weigh(queries):
        scores = lax.dot_general(
            queries, k_all[...], (((1,), (1,)), ((), ())), preferred_element_type=F32
        )
        live = lax.broadcasted_iota(jnp.int32, scores.shape, 1) < image_keys + length
        scores = jnp.where(live, scores, NEG_LARGE)
        peak = jnp.max(scores, axis=1, keepdims=True)
        weights = jnp.where(live, jnp.exp((scores - peak) * scale), 0.0)
        return weights.astype(BF16), jnp.sum(weights, axis=1, keepdims=True)

    def blend(weights, total):
        return jnp.dot(weights, v_all[...], preferred_element_type=F32) / total

    over(n, lambda o: k_copy((p + o) % n, (p + n - o) % n).wait_recv())
    text_weights, text_total = weigh(txt_ref[0, pl.ds(pl.multiple_of(group * share, share), share), :])
    over(n, lambda o: v_copy((p + o) % n, (p + n - o) % n).wait_recv())
    text_done = blend(text_weights, text_total)
    text_row = lax.broadcasted_iota(jnp.int32, text_done.shape, 0) + group * share
    text_done = jnp.where(text_row < length, text_done, 0.0).astype(BF16)

    def block(s):
        return txt_out.at[
            pl.ds(pl.multiple_of((s % groups) * share, share), share), cols(s // groups)
        ]

    def line_copy(o, s):
        return pltpu.make_async_remote_copy(
            t_send, block(s), t1_ss.at[o], t_rs.at[s], device_id={"seq": (p + o * plane) % n}
        )

    def plane_copy(i, o, s):
        source = t_send if i is None else block(s)
        slot = 0 if i is None else i
        return pltpu.make_async_remote_copy(
            source, block(s), t2_ss.at[slot, o], t_rs.at[s],
            device_id={"seq": (p // plane) * plane + (p % plane + o) % plane},
        )

    t_send[...] = text_done
    txt_out[pl.ds(pl.multiple_of(group * share, share), share), cols(head)] = text_done
    over(lines, lambda o: line_copy(o, p).start())
    over(plane, lambda o: plane_copy(None, o, p).start())

    over(heads, lambda o: q_copy((head + o) % heads, (head + heads - o) % heads).wait_recv())
    a_send[...] = blend(*weigh(q_all[...])).astype(BF16)
    over(heads, lambda o: a_copy((head + o) % heads, head).start())
    home[:, cols(head)] = a_send[rows(head), :]

    def forward(i):
        s = (p + n - i * plane) % n
        line_copy(i, s).wait_recv()
        over(plane, lambda o: plane_copy(i, o, s).start())

    over(lines, forward)

    over(heads, lambda o: a_copy((head + o) % heads, (head + heads - o) % heads).wait_recv())
    for load in loads:
        load.wait()

    def p_copy(c):
        return pltpu.make_async_remote_copy(
            p_send.at[c], p_recv.at[c], p_ss.at[c], p_rs.at[c], device_id={"tp": 1 - t}
        )

    mine = []
    for c in range(chunks):
        part = jnp.dot(home[...], w[:, c * width : (c + 1) * width], preferred_element_type=F32)
        top, bottom = part[:half], part[half:]
        p_send[c] = jnp.where(t == 0, bottom, top).astype(BF16)
        p_copy(c).start()
        at = slice(c * width, (c + 1) * width)
        mine.append(jnp.where(t == 0, top, bottom))
    for c in range(chunks):
        at = slice(c * width, (c + 1) * width)
        p_copy(c).wait_recv()
        projected = mine[c] + p_recv[c].astype(F32)
        out_ref[:, at] = (
            res[:, at].astype(F32) + gate[:, at] * (projected + bias[:, at])
        ).astype(BF16)

    def finish_line(i):
        s = (p + n - i * plane) % n
        over(plane, lambda o: plane_copy(i, o, s).wait_send())
        line_copy(i, s).wait_send()

    def finish_plane(o):
        def one(i, carry):
            s = i * plane + (p % plane + o) % plane
            plane_copy(None, o, s).wait_recv()
            return carry

        lax.fori_loop(0, lines, one, 0)
        plane_copy(None, o, p).wait_send()

    over(plane, finish_plane)
    over(lines, finish_line)
    over(n, lambda o: k_copy((p + o) % n, p).wait_send())
    over(n, lambda o: v_copy((p + o) % n, p).wait_send())
    over(heads, lambda o: q_copy((head + o) % heads, head).wait_send())
    over(heads, lambda o: a_copy((head + o) % heads, head).wait_send())
    for c in range(chunks):
        p_copy(c).wait_send()


def shards(img_qkv, txt_qkv, frame_index, row_index, column_index, txt_len, residual, w_proj, proj_bias, gate):
    tokens = img_qkv.shape[1]
    channels = img_qkv.shape[3]
    heads = channels // HD
    n = lax.axis_size("seq")
    groups = n // heads
    text = txt_qkv.shape[1]
    share = text // groups
    plane = largest_divisor(n)
    lines = n // plane
    model = w_proj.shape[1]
    half = residual.shape[1]
    chunks = 4
    head = lax.axis_index("seq") // groups
    img = img_qkv[0].transpose(1, 0, 2)
    txt = lax.dynamic_slice_in_dim(txt_qkv[0], head * HD, HD, 2).transpose(1, 0, 2)
    positions = jnp.concatenate([frame_index, row_index, column_index], axis=0)
    vmem = pl.BlockSpec(memory_space=pltpu.VMEM)
    anyspace = pl.BlockSpec(memory_space=pl.ANY)
    dma = pltpu.SemaphoreType.DMA
    out, txt_out = pl.pallas_call(
        functools.partial(kernel, n, heads),
        out_shape=(
            jax.ShapeDtypeStruct((half, model), BF16),
            jax.ShapeDtypeStruct((text, channels), BF16),
        ),
        in_specs=[vmem, vmem, vmem, vmem, pl.BlockSpec(memory_space=pltpu.SMEM)] + [anyspace] * 4,
        out_specs=(vmem, vmem),
        scratch_shapes=[
            pltpu.VMEM((heads, tokens, HD), BF16),
            pltpu.VMEM((heads, tokens, HD), BF16),
            pltpu.VMEM((heads * tokens, HD), BF16),
            pltpu.VMEM((n * tokens + text, HD), BF16),
            pltpu.VMEM((n * tokens + text, HD), BF16),
            pltpu.VMEM((heads * tokens, HD), BF16),
            pltpu.VMEM((tokens, channels), BF16),
            pltpu.VMEM((share, HD), BF16),
            pltpu.VMEM(w_proj.shape, BF16),
            pltpu.VMEM((half, model), BF16),
            pltpu.VMEM((1, model), F32),
            pltpu.VMEM((1, model), F32),
            pltpu.VMEM((chunks, half, model // chunks), BF16),
            pltpu.VMEM((chunks, half, model // chunks), BF16),
            dma((4,)),
            dma((heads,)), dma((heads,)),
            dma((n,)), dma((n,)),
            dma((n,)), dma((n,)),
            dma((heads,)), dma((heads,)),
            dma((lines,)), dma((lines, plane)), dma((n,)),
            dma((chunks,)), dma((chunks,)),
        ],
        compiler_params=pltpu.CompilerParams(
            collective_id=0, has_side_effects=True, vmem_limit_bytes=48 * 1024 * 1024
        ),
    )(
        img, txt, positions, jnp.asarray(pair_rates()), txt_len, residual[0], w_proj,
        proj_bias[None], gate[None],
    )
    return out[None], txt_out[None]


def solution(mesh):
    in_specs = (
        P(None, "seq", None, "tp"),
        P(None, None, None, "tp"),
        P(None, "seq"),
        P(None, "seq"),
        P(None, "seq"),
        P(),
        P(None, ("seq", "tp"), None),
        P("tp", None),
        P(),
        P(),
    )
    out_specs = (P(None, ("seq", "tp"), None), P(None, None, "tp"))
    return jax.shard_map(shards, mesh=mesh, in_specs=in_specs, out_specs=out_specs, check_vma=False)
```

```python
import functools
import math

import jax
import jax.numpy as jnp
from jax import lax
from jax.experimental import pallas as pl
from jax.experimental.pallas import tpu as pltpu
from jax.sharding import PartitionSpec as P

HD = 128
ROPE_BASE_LOG2 = 8.0
NEG_LARGE = -1e30
F32 = jnp.float32
BF16 = jnp.bfloat16


def largest_divisor(n):
    best = 1
    for d in range(1, n + 1):
        if n % d == 0 and d * d <= n:
            best = d
    return best


def kernel(
    n, heads, img_hbm, txt_hbm, frame_hbm, row_hbm, column_hbm, len_ref, res_hbm, w_hbm, bias_hbm, gate_hbm,
    out_ref, txt_out,
    img_ref, txt_q, places, q_send, k_send, q_all, k_all, v_all, a_send, home, t_send, w, res, bias, gate, p_send, p_recv,
    local_sem, q_ss, q_rs, k_ss, k_rs, v_ss, v_rs, a_ss, a_rs, t1_ss, t2_ss, t_rs, p_ss, p_rs,
):
    p = lax.axis_index("seq")
    t = lax.axis_index("tp")
    groups = n // heads
    head = p // groups
    group = p % groups
    tokens = img_ref.shape[1]
    text = txt_hbm.shape[1]
    share = text // groups
    image_keys = n * tokens
    scale = 1.0 / math.sqrt(HD)
    chunks = p_send.shape[0]
    width = p_send.shape[2]
    half = tokens // 2
    plane = largest_divisor(n)
    lines = n // plane

    def rows(s):
        return pl.ds(pl.multiple_of(s * tokens, tokens), tokens)

    def cols(h):
        return pl.ds(pl.multiple_of(h * HD, HD), HD)

    text_rows = pl.ds(pl.multiple_of(group * share, share), share)
    text_keys = pl.ds(image_keys, text)
    early, middle, late = (
        [pltpu.make_async_copy(src, dst, local_sem.at[first + i]) for i, (src, dst) in enumerate(pairs)]
        for first, pairs in (
            (
                0,
                (
                    (frame_hbm, places.at[0]),
                    (row_hbm, places.at[1]),
                    (column_hbm, places.at[2]),
                    (img_hbm, img_ref),
                ),
            ),
            (
                4,
                (
                    (txt_hbm.at[0, text_rows, cols(head)], txt_q),
                    (txt_hbm.at[1, :, cols(head)], k_all.at[text_keys]),
                    (txt_hbm.at[2, :, cols(head)], v_all.at[text_keys]),
                ),
            ),
            (7, ((w_hbm, w), (res_hbm, res), (bias_hbm, bias), (gate_hbm, gate))),
        )
    )
    for load in early + middle + late:
        load.start()

    barrier = pltpu.get_barrier_semaphore()

    def greet(o, carry):
        pl.semaphore_signal(barrier, inc=1, device_id={"seq": (p + o) % n})
        return carry

    lax.fori_loop(1, n, greet, 0)
    pl.semaphore_signal(barrier, inc=1, device_id={"tp": 1 - t})

    diagonal = lax.broadcasted_iota(jnp.int32, (tokens, tokens), 0) == lax.broadcasted_iota(
        jnp.int32, (tokens, tokens), 1
    )
    channel = lax.broadcasted_iota(jnp.int32, (1, HD), 1)
    first = HD // 8
    second = (HD - first) // 2
    angles = jnp.zeros((tokens, HD), F32)
    for load in early:
        load.wait()
    for part, (start, size) in enumerate(
        ((0, first), (first, second), (first + second, second))
    ):
        inside = (channel >= start) & (channel < start + size)
        pair = ((channel - start) // 2).astype(F32)
        rate = jnp.where(inside, jnp.exp2(pair * (-2.0 * ROPE_BASE_LOG2 / size)), 0.0)
        column = jnp.sum(
            jnp.where(diagonal, places[part].astype(F32), 0.0), axis=1, keepdims=True
        )
        angles = angles + column * rate
    even = lax.broadcasted_iota(jnp.int32, (tokens, HD), 1) % 2 == 0
    cosine = jnp.cos(angles)
    sine = jnp.where(even, -1.0, 1.0) * jnp.sin(angles)
    for which, dst in ((0, q_send), (1, k_send)):
        for h in range(heads):
            x = img_ref[which, :, h * HD : (h + 1) * HD].astype(F32)
            partner = jnp.where(even, pltpu.roll(x, HD - 1, 1), pltpu.roll(x, 1, 1))
            dst[h] = (x * cosine + partner * sine).astype(BF16)

    pl.semaphore_wait(barrier, n)

    def q_copy(h, src_line):
        return pltpu.make_async_remote_copy(
            q_send.at[h], q_all.at[rows(src_line)], q_ss.at[h], q_rs.at[src_line],
            device_id={"seq": h * groups + group},
        )

    def k_copy(d, s):
        return pltpu.make_async_remote_copy(
            k_send.at[d // groups], k_all.at[rows(s)], k_ss.at[d], k_rs.at[s], device_id={"seq": d}
        )

    def v_copy(d, s):
        return pltpu.make_async_remote_copy(
            img_ref.at[2, :, cols(d // groups)], v_all.at[rows(s)], v_ss.at[d], v_rs.at[s],
            device_id={"seq": d},
        )

    def a_copy(j, h):
        return pltpu.make_async_remote_copy(
            a_send.at[rows(j)], home.at[:, cols(h)], a_ss.at[j], a_rs.at[h],
            device_id={"seq": j * groups + group},
        )

    def over(count, f):
        def step(o, carry):
            f(o)
            return carry

        lax.fori_loop(1, count, step, 0)

    over(n, lambda o: k_copy((p + o) % n, p).start())
    over(heads, lambda o: q_copy((head + o) % heads, head).start())
    over(n, lambda o: v_copy((p + o) % n, p).start())

    q_all[rows(head), :] = q_send[head]
    k_all[rows(p), :] = k_send[head]
    v_all[rows(p), :] = img_ref[2, :, cols(head)]
    for load in middle:
        load.wait()
    length = len_ref[0]

    def weigh(queries):
        scores = lax.dot_general(
            queries, k_all[...], (((1,), (1,)), ((), ())), preferred_element_type=F32
        )
        live = lax.broadcasted_iota(jnp.int32, scores.shape, 1) < image_keys + length
        scores = jnp.where(live, scores, NEG_LARGE)
        peak = jnp.max(scores, axis=1, keepdims=True)
        weights = jnp.where(live, jnp.exp((scores - peak) * scale), 0.0)
        return weights.astype(BF16), jnp.sum(weights, axis=1, keepdims=True)

    def blend(weights, total):
        return jnp.dot(weights, v_all[...], preferred_element_type=F32) / total

    over(n, lambda o: k_copy((p + o) % n, (p + n - o) % n).wait_recv())
    text_weights, text_total = weigh(txt_q[...])
    over(heads, lambda o: q_copy((head + o) % heads, (head + heads - o) % heads).wait_recv())
    image_weights, image_total = weigh(q_all[...])
    over(n, lambda o: v_copy((p + o) % n, (p + n - o) % n).wait_recv())
    text_done = blend(text_weights, text_total)
    text_row = lax.broadcasted_iota(jnp.int32, text_done.shape, 0) + group * share
    text_done = jnp.where(text_row < length, text_done, 0.0).astype(BF16)

    def block(s):
        return txt_out.at[
            pl.ds(pl.multiple_of((s % groups) * share, share), share), cols(s // groups)
        ]

    def line_copy(o, s):
        return pltpu.make_async_remote_copy(
            t_send, block(s), t1_ss.at[o], t_rs.at[s], device_id={"seq": (p + o * plane) % n}
        )

    def plane_copy(i, o, s):
        source = t_send if i is None else block(s)
        slot = 0 if i is None else i
        return pltpu.make_async_remote_copy(
            source, block(s), t2_ss.at[slot, o], t_rs.at[s],
            device_id={"seq": (p // plane) * plane + (p % plane + o) % plane},
        )

    t_send[...] = text_done
    txt_out[pl.ds(pl.multiple_of(group * share, share), share), cols(head)] = text_done
    over(lines, lambda o: line_copy(o, p).start())
    over(plane, lambda o: plane_copy(None, o, p).start())

    a_send[...] = blend(image_weights, image_total).astype(BF16)
    over(heads, lambda o: a_copy((head + o) % heads, head).start())
    home[:, cols(head)] = a_send[rows(head), :]

    def forward(i):
        s = (p + n - i * plane) % n
        line_copy(i, s).wait_recv()
        over(plane, lambda o: plane_copy(i, o, s).start())

    over(lines, forward)

    over(heads, lambda o: a_copy((head + o) % heads, (head + heads - o) % heads).wait_recv())
    for load in late:
        load.wait()

    def p_copy(c):
        return pltpu.make_async_remote_copy(
            p_send.at[c], p_recv.at[c], p_ss.at[c], p_rs.at[c], device_id={"tp": 1 - t}
        )

    mine = []
    for c in range(chunks):
        part = jnp.dot(home[...], w[:, c * width : (c + 1) * width], preferred_element_type=F32)
        top, bottom = part[:half], part[half:]
        p_send[c] = jnp.where(t == 0, bottom, top).astype(BF16)
        p_copy(c).start()
        at = slice(c * width, (c + 1) * width)
        mine.append(jnp.where(t == 0, top, bottom))
    for c in range(chunks):
        at = slice(c * width, (c + 1) * width)
        p_copy(c).wait_recv()
        projected = mine[c] + p_recv[c].astype(F32)
        out_ref[:, at] = (
            res[:, at].astype(F32) + gate[:, at] * (projected + bias[:, at])
        ).astype(BF16)

    def finish_line(i):
        s = (p + n - i * plane) % n
        over(plane, lambda o: plane_copy(i, o, s).wait_send())
        line_copy(i, s).wait_send()

    def finish_plane(o):
        def one(i, carry):
            s = i * plane + (p % plane + o) % plane
            plane_copy(None, o, s).wait_recv()
            return carry

        lax.fori_loop(0, lines, one, 0)
        plane_copy(None, o, p).wait_send()

    over(plane, finish_plane)
    over(lines, finish_line)
    over(n, lambda o: k_copy((p + o) % n, p).wait_send())
    over(n, lambda o: v_copy((p + o) % n, p).wait_send())
    over(heads, lambda o: q_copy((head + o) % heads, head).wait_send())
    over(heads, lambda o: a_copy((head + o) % heads, head).wait_send())
    for c in range(chunks):
        p_copy(c).wait_send()


def store(img_ref, txt_ref, img_hbm, txt_hbm, sem):
    copies = [
        pltpu.make_async_copy(txt_ref, txt_hbm.at[0], sem.at[0]),
        pltpu.make_async_copy(img_ref, img_hbm.at[0], sem.at[1]),
    ]
    for copy in copies:
        copy.start()
    for copy in copies:
        copy.wait()


def shards(img_qkv, txt_qkv, frame_index, row_index, column_index, txt_len, residual, w_proj, proj_bias, gate):
    tokens = img_qkv.shape[1]
    channels = img_qkv.shape[3]
    heads = channels // HD
    n = lax.axis_size("seq")
    groups = n // heads
    text = txt_qkv.shape[1]
    share = text // groups
    plane = largest_divisor(n)
    lines = n // plane
    model = w_proj.shape[1]
    half = residual.shape[1]
    chunks = 4
    img = img_qkv[0].transpose(1, 0, 2)
    txt = txt_qkv[0].transpose(1, 0, 2)
    vmem = pl.BlockSpec(memory_space=pltpu.VMEM)
    hbm = pl.BlockSpec(memory_space=pltpu.HBM)
    dma = pltpu.SemaphoreType.DMA
    out, txt_out = pl.pallas_call(
        functools.partial(kernel, n, heads),
        out_shape=(
            jax.ShapeDtypeStruct((half, model), BF16),
            jax.ShapeDtypeStruct((text, channels), BF16),
        ),
        in_specs=[hbm] * 5 + [pl.BlockSpec(memory_space=pltpu.SMEM)] + [hbm] * 4,
        out_specs=(vmem, vmem),
        scratch_shapes=[
            pltpu.VMEM((3, tokens, channels), BF16),
            pltpu.VMEM((share, HD), BF16),
            pltpu.VMEM((3, 1, tokens), jnp.int32),
            pltpu.VMEM((heads, tokens, HD), BF16),
            pltpu.VMEM((heads, tokens, HD), BF16),
            pltpu.VMEM((heads * tokens, HD), BF16),
            pltpu.VMEM((n * tokens + text, HD), BF16),
            pltpu.VMEM((n * tokens + text, HD), BF16),
            pltpu.VMEM((heads * tokens, HD), BF16),
            pltpu.VMEM((tokens, channels), BF16),
            pltpu.VMEM((share, HD), BF16),
            pltpu.VMEM(w_proj.shape, BF16),
            pltpu.VMEM((half, model), BF16),
            pltpu.VMEM((1, model), F32),
            pltpu.VMEM((1, model), F32),
            pltpu.VMEM((chunks, half, model // chunks), BF16),
            pltpu.VMEM((chunks, half, model // chunks), BF16),
            dma((11,)),
            dma((heads,)), dma((heads,)),
            dma((n,)), dma((n,)),
            dma((n,)), dma((n,)),
            dma((heads,)), dma((heads,)),
            dma((lines,)), dma((lines, plane)), dma((n,)),
            dma((chunks,)), dma((chunks,)),
        ],
        compiler_params=pltpu.CompilerParams(
            collective_id=0, has_side_effects=True, vmem_limit_bytes=67043328
        ),
    )(
        img, txt, frame_index, row_index, column_index, txt_len, residual[0], w_proj,
        proj_bias[None], gate[None],
    )
    return pl.pallas_call(
        store,
        out_shape=(
            jax.ShapeDtypeStruct((1,) + out.shape, BF16),
            jax.ShapeDtypeStruct((1,) + txt_out.shape, BF16),
        ),
        in_specs=[vmem, vmem],
        out_specs=(hbm, hbm),
        scratch_shapes=[dma((2,))],
        compiler_params=pltpu.CompilerParams(vmem_limit_bytes=66400000),
    )(out, txt_out)


def solution(mesh):
    in_specs = (
        P(None, "seq", None, "tp"),
        P(None, None, None, "tp"),
        P(None, "seq"),
        P(None, "seq"),
        P(None, "seq"),
        P(),
        P(None, ("seq", "tp"), None),
        P("tp", None),
        P(),
        P(),
    )
    out_specs = (P(None, ("seq", "tp"), None), P(None, None, "tp"))
    return jax.shard_map(shards, mesh=mesh, in_specs=in_specs, out_specs=out_specs, check_vma=False)
```

```python
import functools
import math

import jax
import jax.numpy as jnp
from jax import lax
from jax.experimental import pallas as pl
from jax.experimental.pallas import tpu as pltpu
from jax.sharding import PartitionSpec as P

HD = 128
ROPE_BASE_LOG2 = 8.0
NEG_LARGE = -1e30
F32 = jnp.float32
BF16 = jnp.bfloat16


def largest_divisor(n):
    best = 1
    for d in range(1, n + 1):
        if n % d == 0 and d * d <= n:
            best = d
    return best


def kernel(
    n, heads, img_hbm, txt_hbm, frame_hbm, row_hbm, column_hbm, len_ref, res_hbm, w_hbm, bias_hbm, gate_hbm,
    out_hbm, txt_out_hbm,
    out_ref, txt_out,
    img_ref, txt_q, places, q_send, k_send, q_all, k_all, v_all, a_send, home, t_send, w, res, bias, gate, p_send, p_recv,
    local_sem, q_ss, q_rs, k_ss, k_rs, kr_ss, v_ss, v_rs, vr_ss, a_ss, a_rs, t1_ss, t2_ss, t_rs, p_ss, p_rs,
):
    p = lax.axis_index("seq")
    t = lax.axis_index("tp")
    groups = n // heads
    head = p // groups
    group = p % groups
    tokens = img_ref.shape[1]
    text = txt_hbm.shape[1]
    share = text // groups
    image_keys = n * tokens
    scale = 1.0 / math.sqrt(HD)
    chunks = p_send.shape[0]
    width = p_send.shape[2]
    half = tokens // 2
    plane = largest_divisor(n)
    lines = n // plane

    def rows(s):
        return pl.ds(pl.multiple_of(s * tokens, tokens), tokens)

    def cols(h):
        return pl.ds(pl.multiple_of(h * HD, HD), HD)

    text_rows = pl.ds(pl.multiple_of(group * share, share), share)
    text_keys = pl.ds(image_keys, text)
    early, middle, late = (
        [pltpu.make_async_copy(src, dst, local_sem.at[first + i]) for i, (src, dst) in enumerate(pairs)]
        for first, pairs in (
            (
                0,
                (
                    (frame_hbm, places.at[0]),
                    (row_hbm, places.at[1]),
                    (column_hbm, places.at[2]),
                    (img_hbm, img_ref),
                ),
            ),
            (
                4,
                (
                    (txt_hbm.at[0, text_rows, cols(head)], txt_q),
                    (txt_hbm.at[1, :, cols(head)], k_all.at[text_keys]),
                    (txt_hbm.at[2, :, cols(head)], v_all.at[text_keys]),
                ),
            ),
            (7, ((w_hbm, w), (res_hbm, res), (bias_hbm, bias), (gate_hbm, gate))),
        )
    )
    for load in early + middle + late:
        load.start()

    barrier = pltpu.get_barrier_semaphore()

    def greet(o, carry):
        pl.semaphore_signal(barrier, inc=1, device_id={"seq": (p + o) % n})
        return carry

    lax.fori_loop(1, n, greet, 0)
    pl.semaphore_signal(barrier, inc=1, device_id={"tp": 1 - t})

    diagonal = lax.broadcasted_iota(jnp.int32, (tokens, tokens), 0) == lax.broadcasted_iota(
        jnp.int32, (tokens, tokens), 1
    )
    channel = lax.broadcasted_iota(jnp.int32, (1, HD), 1)
    first = HD // 8
    second = (HD - first) // 2
    angles = jnp.zeros((tokens, HD), F32)
    for load in early:
        load.wait()
    for part, (start, size) in enumerate(
        ((0, first), (first, second), (first + second, second))
    ):
        inside = (channel >= start) & (channel < start + size)
        pair = ((channel - start) // 2).astype(F32)
        rate = jnp.where(inside, jnp.exp2(pair * (-2.0 * ROPE_BASE_LOG2 / size)), 0.0)
        column = jnp.sum(
            jnp.where(diagonal, places[part].astype(F32), 0.0), axis=1, keepdims=True
        )
        angles = angles + column * rate
    even = lax.broadcasted_iota(jnp.int32, (tokens, HD), 1) % 2 == 0
    cosine = jnp.cos(angles)
    sine = jnp.where(even, -1.0, 1.0) * jnp.sin(angles)
    for which, dst in ((0, q_send), (1, k_send)):
        for h in range(heads):
            x = img_ref[which, :, h * HD : (h + 1) * HD].astype(F32)
            partner = jnp.where(even, pltpu.roll(x, HD - 1, 1), pltpu.roll(x, 1, 1))
            dst[h] = (x * cosine + partner * sine).astype(BF16)

    pl.semaphore_wait(barrier, n)

    def q_copy(h, src_line):
        return pltpu.make_async_remote_copy(
            q_send.at[h], q_all.at[rows(src_line)], q_ss.at[h], q_rs.at[src_line],
            device_id={"seq": h * groups + group},
        )

    def k_copy(h, s):
        return pltpu.make_async_remote_copy(
            k_send.at[h], k_all.at[rows(s)], k_ss.at[h], k_rs.at[s],
            device_id={"seq": h * groups + group},
        )

    def v_copy(h, s):
        return pltpu.make_async_remote_copy(
            img_ref.at[2, :, cols(h)], v_all.at[rows(s)], v_ss.at[h], v_rs.at[s],
            device_id={"seq": h * groups + group},
        )

    def k_relay(j, o, s):
        return pltpu.make_async_remote_copy(
            k_all.at[rows(s)], k_all.at[rows(s)], kr_ss.at[j, o], k_rs.at[s],
            device_id={"seq": head * groups + (group + o) % groups},
        )

    def v_relay(j, o, s):
        return pltpu.make_async_remote_copy(
            v_all.at[rows(s)], v_all.at[rows(s)], vr_ss.at[j, o], v_rs.at[s],
            device_id={"seq": head * groups + (group + o) % groups},
        )

    def a_copy(j, h):
        return pltpu.make_async_remote_copy(
            a_send.at[rows(j)], home.at[:, cols(h)], a_ss.at[j], a_rs.at[h],
            device_id={"seq": j * groups + group},
        )

    def over(count, f):
        def step(o, carry):
            f(o)
            return carry

        lax.fori_loop(1, count, step, 0)

    over(heads, lambda o: k_copy((head + o) % heads, p).start())
    k_all[rows(p), :] = k_send[head]
    over(groups, lambda o: k_relay(head, o, p).start())
    over(heads, lambda o: v_copy((head + o) % heads, p).start())
    v_all[rows(p), :] = img_ref[2, :, cols(head)]
    over(groups, lambda o: v_relay(head, o, p).start())
    over(heads, lambda o: q_copy((head + o) % heads, head).start())
    q_all[rows(head), :] = q_send[head]

    def pass_on(copy, relay):
        def one(o):
            j = (head + heads - o) % heads
            s = j * groups + group
            copy((head + o) % heads, s).wait_recv()
            over(groups, lambda g: relay(j, g, s).start())

        over(heads, one)

    def arrive(relay):
        def one(o):
            def from_line(j, carry):
                relay(j, o, j * groups + (group + o) % groups).wait_recv()
                return carry

            lax.fori_loop(0, heads, from_line, 0)

        over(groups, one)

    pass_on(k_copy, k_relay)
    pass_on(v_copy, v_relay)
    for load in middle:
        load.wait()
    length = len_ref[0]

    def weigh(queries):
        scores = lax.dot_general(
            queries, k_all[...], (((1,), (1,)), ((), ())), preferred_element_type=F32
        )
        live = lax.broadcasted_iota(jnp.int32, scores.shape, 1) < image_keys + length
        scores = jnp.where(live, scores, NEG_LARGE)
        peak = jnp.max(scores, axis=1, keepdims=True)
        weights = jnp.where(live, jnp.exp((scores - peak) * scale), 0.0)
        return weights.astype(BF16), jnp.sum(weights, axis=1, keepdims=True)

    def blend(weights, total):
        return jnp.dot(weights, v_all[...], preferred_element_type=F32) / total

    arrive(k_relay)
    text_weights, text_total = weigh(txt_q[...])
    over(heads, lambda o: q_copy((head + o) % heads, (head + heads - o) % heads).wait_recv())
    image_weights, image_total = weigh(q_all[...])
    arrive(v_relay)
    text_done = blend(text_weights, text_total)
    text_row = lax.broadcasted_iota(jnp.int32, text_done.shape, 0) + group * share
    text_done = jnp.where(text_row < length, text_done, 0.0).astype(BF16)

    def block(s):
        return txt_out.at[
            pl.ds(pl.multiple_of((s % groups) * share, share), share), cols(s // groups)
        ]

    def line_copy(o, s):
        return pltpu.make_async_remote_copy(
            t_send, block(s), t1_ss.at[o], t_rs.at[s], device_id={"seq": (p + o * plane) % n}
        )

    def plane_copy(i, o, s):
        source = t_send if i is None else block(s)
        slot = 0 if i is None else i
        return pltpu.make_async_remote_copy(
            source, block(s), t2_ss.at[slot, o], t_rs.at[s],
            device_id={"seq": (p // plane) * plane + (p % plane + o) % plane},
        )

    t_send[...] = text_done
    txt_out[pl.ds(pl.multiple_of(group * share, share), share), cols(head)] = text_done
    over(lines, lambda o: line_copy(o, p).start())
    over(plane, lambda o: plane_copy(None, o, p).start())

    a_send[...] = blend(image_weights, image_total).astype(BF16)
    over(heads, lambda o: a_copy((head + o) % heads, head).start())
    home[:, cols(head)] = a_send[rows(head), :]

    def forward(i):
        s = (p + n - i * plane) % n
        line_copy(i, s).wait_recv()
        over(plane, lambda o: plane_copy(i, o, s).start())

    over(lines, forward)

    over(heads, lambda o: a_copy((head + o) % heads, (head + heads - o) % heads).wait_recv())
    for load in late:
        load.wait()

    def p_copy(c):
        return pltpu.make_async_remote_copy(
            p_send.at[c], p_recv.at[c], p_ss.at[c], p_rs.at[c], device_id={"tp": 1 - t}
        )

    mine = []
    for c in range(chunks):
        part = jnp.dot(home[...], w[:, c * width : (c + 1) * width], preferred_element_type=F32)
        top, bottom = part[:half], part[half:]
        p_send[c] = jnp.where(t == 0, bottom, top).astype(BF16)
        p_copy(c).start()
        at = slice(c * width, (c + 1) * width)
        mine.append(jnp.where(t == 0, top, bottom))
    def finish_plane(o):
        def one(i, carry):
            s = i * plane + (p % plane + o) % plane
            plane_copy(None, o, s).wait_recv()
            return carry

        lax.fori_loop(0, lines, one, 0)
        plane_copy(None, o, p).wait_send()

    over(plane, finish_plane)
    stores = [
        pltpu.make_async_copy(src, dst, local_sem.at[11 + i])
        for i, (src, dst) in enumerate(((txt_out, txt_out_hbm), (out_ref, out_hbm)))
    ]
    stores[0].start()
    for c in range(chunks):
        at = slice(c * width, (c + 1) * width)
        p_copy(c).wait_recv()
        projected = mine[c] + p_recv[c].astype(F32)
        out_ref[:, at] = (
            res[:, at].astype(F32) + gate[:, at] * (projected + bias[:, at])
        ).astype(BF16)
    stores[1].start()

    def finish_line(i):
        s = (p + n - i * plane) % n
        over(plane, lambda o: plane_copy(i, o, s).wait_send())
        line_copy(i, s).wait_send()

    over(lines, finish_line)
    def finish_relay(relay):
        def one(o):
            def to_line(j, carry):
                relay(j, o, j * groups + group).wait_send()
                return carry

            lax.fori_loop(0, heads, to_line, 0)

        over(groups, one)

    finish_relay(k_relay)
    finish_relay(v_relay)
    over(heads, lambda o: k_copy((head + o) % heads, p).wait_send())
    over(heads, lambda o: v_copy((head + o) % heads, p).wait_send())
    over(heads, lambda o: q_copy((head + o) % heads, head).wait_send())
    over(heads, lambda o: a_copy((head + o) % heads, head).wait_send())
    for c in range(chunks):
        p_copy(c).wait_send()
    for copy in stores:
        copy.wait()


def store(img_in, txt_in, img_out, txt_out, img, txt, load_sem, store_sem):
    pieces = load_sem.shape[0] - 1
    rows = txt.shape[0] // pieces
    parts = [(txt_in.at[pl.ds(i * rows, rows)], txt.at[pl.ds(i * rows, rows)],
              txt_out.at[0, pl.ds(i * rows, rows)]) for i in range(pieces)]
    parts.append((img_in, img, img_out.at[0]))
    loads = [pltpu.make_async_copy(a, b, load_sem.at[i]) for i, (a, b, c) in enumerate(parts)]
    stores = [pltpu.make_async_copy(b, c, store_sem.at[i]) for i, (a, b, c) in enumerate(parts)]
    for load in loads:
        load.start()
    for load, put in zip(loads, stores):
        load.wait()
        put.start()
    for put in stores:
        put.wait()


def shards(img_qkv, txt_qkv, frame_index, row_index, column_index, txt_len, residual, w_proj, proj_bias, gate):
    tokens = img_qkv.shape[1]
    channels = img_qkv.shape[3]
    heads = channels // HD
    n = lax.axis_size("seq")
    groups = n // heads
    text = txt_qkv.shape[1]
    share = text // groups
    plane = largest_divisor(n)
    lines = n // plane
    model = w_proj.shape[1]
    half = residual.shape[1]
    chunks = 4
    img = img_qkv[0].transpose(1, 0, 2)
    txt = txt_qkv[0].transpose(1, 0, 2)
    hbm = pl.BlockSpec(memory_space=pltpu.HBM)
    dma = pltpu.SemaphoreType.DMA
    out, txt_out = pl.pallas_call(
        functools.partial(kernel, n, heads),
        out_shape=(
            jax.ShapeDtypeStruct((half, model), BF16),
            jax.ShapeDtypeStruct((text, channels), BF16),
        ),
        in_specs=[hbm] * 5 + [pl.BlockSpec(memory_space=pltpu.SMEM)] + [hbm] * 4,
        out_specs=(hbm, hbm),
        scratch_shapes=[
            pltpu.VMEM((half, model), BF16),
            pltpu.VMEM((text, channels), BF16),
            pltpu.VMEM((3, tokens, channels), BF16),
            pltpu.VMEM((share, HD), BF16),
            pltpu.VMEM((3, 1, tokens), jnp.int32),
            pltpu.VMEM((heads, tokens, HD), BF16),
            pltpu.VMEM((heads, tokens, HD), BF16),
            pltpu.VMEM((heads * tokens, HD), BF16),
            pltpu.VMEM((n * tokens + text, HD), BF16),
            pltpu.VMEM((n * tokens + text, HD), BF16),
            pltpu.VMEM((heads * tokens, HD), BF16),
            pltpu.VMEM((tokens, channels), BF16),
            pltpu.VMEM((share, HD), BF16),
            pltpu.VMEM(w_proj.shape, BF16),
            pltpu.VMEM((half, model), BF16),
            pltpu.VMEM((1, model), F32),
            pltpu.VMEM((1, model), F32),
            pltpu.VMEM((chunks, half, model // chunks), BF16),
            pltpu.VMEM((chunks, half, model // chunks), BF16),
            dma((13,)),
            dma((heads,)), dma((heads,)),
            dma((heads,)), dma((n,)), dma((heads, groups)),
            dma((heads,)), dma((n,)), dma((heads, groups)),
            dma((heads,)), dma((heads,)),
            dma((lines,)), dma((lines, plane)), dma((n,)),
            dma((chunks,)), dma((chunks,)),
        ],
        compiler_params=pltpu.CompilerParams(
            collective_id=0, has_side_effects=True, vmem_limit_bytes=67043328
        ),
    )(
        img, txt, frame_index, row_index, column_index, txt_len, residual[0], w_proj,
        proj_bias[None], gate[None],
    )
    return pl.pallas_call(
        store,
        out_shape=(
            jax.ShapeDtypeStruct((1,) + out.shape, BF16),
            jax.ShapeDtypeStruct((1,) + txt_out.shape, BF16),
        ),
        in_specs=[hbm, hbm],
        out_specs=(hbm, hbm),
        scratch_shapes=[
            pltpu.VMEM(out.shape, BF16), pltpu.VMEM(txt_out.shape, BF16), dma((5,)), dma((5,)),
        ],
        compiler_params=pltpu.CompilerParams(vmem_limit_bytes=66400000),
    )(out, txt_out)


def solution(mesh):
    in_specs = (
        P(None, "seq", None, "tp"),
        P(None, None, None, "tp"),
        P(None, "seq"),
        P(None, "seq"),
        P(None, "seq"),
        P(),
        P(None, ("seq", "tp"), None),
        P("tp", None),
        P(),
        P(),
    )
    out_specs = (P(None, ("seq", "tp"), None), P(None, None, "tp"))
    return jax.shard_map(shards, mesh=mesh, in_specs=in_specs, out_specs=out_specs, check_vma=False)
```

```python
import functools
import math

import jax
import jax.numpy as jnp
from jax import lax
from jax.experimental import pallas as pl
from jax.experimental.pallas import tpu as pltpu
from jax.sharding import PartitionSpec as P

HD = 128
ROPE_BASE_LOG2 = 8.0
NEG_LARGE = -1e30
F32 = jnp.float32
BF16 = jnp.bfloat16


def largest_divisor(n):
    best = 1
    for d in range(1, n + 1):
        if n % d == 0 and d * d <= n:
            best = d
    return best


def kernel(
    n, heads, img_hbm, txt_hbm, frame_hbm, row_hbm, column_hbm, len_ref, res_hbm, w_hbm, bias_hbm, gate_hbm,
    out_hbm, txt_out_hbm,
    out_ref, txt_out,
    img_ref, txt_q, places, q_send, k_send, q_all, k_all, v_all, a_send, home, t_send, w, res, bias, gate, p_send, p_recv,
    local_sem, q_ss, q_rs, k_ss, k_rs, kr_ss, v_ss, v_rs, vr_ss, a_ss, a_rs, t1_ss, t2_ss, t_rs, p_ss, p_rs,
):
    p = lax.axis_index("seq")
    t = lax.axis_index("tp")
    groups = n // heads
    head = p // groups
    group = p % groups
    tokens = img_ref.shape[1]
    text = txt_hbm.shape[1]
    share = text // groups
    image_keys = n * tokens
    scale = 1.0 / math.sqrt(HD)
    chunks = p_send.shape[0]
    width = p_send.shape[2]
    half = tokens // 2
    plane = largest_divisor(n)
    lines = n // plane

    def rows(s):
        return pl.ds(pl.multiple_of(s * tokens, tokens), tokens)

    def cols(h):
        return pl.ds(pl.multiple_of(h * HD, HD), HD)

    text_rows = pl.ds(pl.multiple_of(group * share, share), share)
    text_keys = pl.ds(image_keys, text)
    early, middle, late = (
        [pltpu.make_async_copy(src, dst, local_sem.at[first + i]) for i, (src, dst) in enumerate(pairs)]
        for first, pairs in (
            (
                0,
                (
                    (frame_hbm, places.at[0]),
                    (row_hbm, places.at[1]),
                    (column_hbm, places.at[2]),
                    (img_hbm, img_ref),
                ),
            ),
            (
                4,
                (
                    (txt_hbm.at[0, text_rows, cols(head)], txt_q),
                    (txt_hbm.at[1, :, cols(head)], k_all.at[text_keys]),
                    (txt_hbm.at[2, :, cols(head)], v_all.at[text_keys]),
                ),
            ),
            (7, ((w_hbm, w), (res_hbm, res), (bias_hbm, bias), (gate_hbm, gate))),
        )
    )
    for load in early + middle + late:
        load.start()

    barrier = pltpu.get_barrier_semaphore()

    def greet(o, carry):
        pl.semaphore_signal(barrier, inc=1, device_id={"seq": (p + o) % n})
        return carry

    lax.fori_loop(1, n, greet, 0)
    pl.semaphore_signal(barrier, inc=1, device_id={"tp": 1 - t})

    diagonal = lax.broadcasted_iota(jnp.int32, (tokens, tokens), 0) == lax.broadcasted_iota(
        jnp.int32, (tokens, tokens), 1
    )
    channel = lax.broadcasted_iota(jnp.int32, (1, HD), 1)
    first = HD // 8
    second = (HD - first) // 2
    angles = jnp.zeros((tokens, HD), F32)
    for load in early:
        load.wait()
    for part, (start, size) in enumerate(
        ((0, first), (first, second), (first + second, second))
    ):
        inside = (channel >= start) & (channel < start + size)
        pair = ((channel - start) // 2).astype(F32)
        rate = jnp.where(inside, jnp.exp2(pair * (-2.0 * ROPE_BASE_LOG2 / size)), 0.0)
        column = jnp.sum(
            jnp.where(diagonal, places[part].astype(F32), 0.0), axis=1, keepdims=True
        )
        angles = angles + column * rate
    even = lax.broadcasted_iota(jnp.int32, (tokens, HD), 1) % 2 == 0
    cosine = jnp.cos(angles)
    sine = jnp.where(even, -1.0, 1.0) * jnp.sin(angles)
    for which, dst in ((0, q_send), (1, k_send)):
        for h in range(heads):
            x = img_ref[which, :, h * HD : (h + 1) * HD].astype(F32)
            partner = jnp.where(even, pltpu.roll(x, HD - 1, 1), pltpu.roll(x, 1, 1))
            dst[h] = (x * cosine + partner * sine).astype(BF16)

    pl.semaphore_wait(barrier, n)

    def q_copy(h, src_line):
        return pltpu.make_async_remote_copy(
            q_send.at[h], q_all.at[rows(src_line)], q_ss.at[h], q_rs.at[src_line],
            device_id={"seq": h * groups + group},
        )

    def k_copy(h, s):
        return pltpu.make_async_remote_copy(
            k_send.at[h], k_all.at[rows(s)], k_ss.at[h], k_rs.at[s],
            device_id={"seq": h * groups + group},
        )

    def v_copy(h, s):
        return pltpu.make_async_remote_copy(
            img_ref.at[2, :, cols(h)], v_all.at[rows(s)], v_ss.at[h], v_rs.at[s],
            device_id={"seq": h * groups + group},
        )

    def k_relay(j, o, s):
        return pltpu.make_async_remote_copy(
            k_all.at[rows(s)], k_all.at[rows(s)], kr_ss.at[j, o], k_rs.at[s],
            device_id={"seq": head * groups + (group + o) % groups},
        )

    def v_relay(j, o, s):
        return pltpu.make_async_remote_copy(
            v_all.at[rows(s)], v_all.at[rows(s)], vr_ss.at[j, o], v_rs.at[s],
            device_id={"seq": head * groups + (group + o) % groups},
        )

    def a_copy(j, h):
        return pltpu.make_async_remote_copy(
            a_send.at[rows(j)], home.at[:, cols(h)], a_ss.at[j], a_rs.at[h],
            device_id={"seq": j * groups + group},
        )

    def over(count, f):
        def step(o, carry):
            f(o)
            return carry

        lax.fori_loop(1, count, step, 0)

    over(heads, lambda o: k_copy((head + o) % heads, p).start())
    k_all[rows(p), :] = k_send[head]
    over(groups, lambda o: k_relay(head, o, p).start())
    over(heads, lambda o: v_copy((head + o) % heads, p).start())
    v_all[rows(p), :] = img_ref[2, :, cols(head)]
    over(groups, lambda o: v_relay(head, o, p).start())
    over(heads, lambda o: q_copy((head + o) % heads, head).start())
    q_all[rows(head), :] = q_send[head]

    def pass_on(copy, relay):
        def one(o):
            j = (head + heads - o) % heads
            s = j * groups + group
            copy((head + o) % heads, s).wait_recv()
            over(groups, lambda g: relay(j, g, s).start())

        over(heads, one)

    def arrive(relay):
        def one(o):
            def from_line(j, carry):
                relay(j, o, j * groups + (group + o) % groups).wait_recv()
                return carry

            lax.fori_loop(0, heads, from_line, 0)

        over(groups, one)

    pass_on(k_copy, k_relay)
    pass_on(v_copy, v_relay)
    for load in middle:
        load.wait()
    length = len_ref[0]

    def weigh(queries):
        scores = lax.dot_general(
            queries, k_all[...], (((1,), (1,)), ((), ())), preferred_element_type=F32
        )
        live = lax.broadcasted_iota(jnp.int32, scores.shape, 1) < image_keys + length
        scores = jnp.where(live, scores, NEG_LARGE)
        peak = jnp.max(scores, axis=1, keepdims=True)
        weights = jnp.where(live, jnp.exp((scores - peak) * scale), 0.0)
        return weights.astype(BF16), jnp.sum(weights, axis=1, keepdims=True)

    def blend(weights, total):
        return jnp.dot(weights, v_all[...], preferred_element_type=F32) / total

    arrive(k_relay)
    text_weights, text_total = weigh(txt_q[...])
    over(heads, lambda o: q_copy((head + o) % heads, (head + heads - o) % heads).wait_recv())
    image_weights, image_total = weigh(q_all[...])
    arrive(v_relay)
    text_done = blend(text_weights, text_total)
    text_row = lax.broadcasted_iota(jnp.int32, text_done.shape, 0) + group * share
    text_done = jnp.where(text_row < length, text_done, 0.0).astype(BF16)

    def block(s):
        return txt_out.at[
            pl.ds(pl.multiple_of((s % groups) * share, share), share), cols(s // groups)
        ]

    def line_copy(o, s):
        return pltpu.make_async_remote_copy(
            t_send, block(s), t1_ss.at[o], t_rs.at[s], device_id={"seq": (p + o * plane) % n}
        )

    def plane_copy(i, o, s):
        source = t_send if i is None else block(s)
        slot = 0 if i is None else i
        return pltpu.make_async_remote_copy(
            source, block(s), t2_ss.at[slot, o], t_rs.at[s],
            device_id={"seq": (p // plane) * plane + (p % plane + o) % plane},
        )

    t_send[...] = text_done
    txt_out[pl.ds(pl.multiple_of(group * share, share), share), cols(head)] = text_done
    over(lines, lambda o: line_copy(o, p).start())
    over(plane, lambda o: plane_copy(None, o, p).start())

    a_send[...] = blend(image_weights, image_total).astype(BF16)
    over(heads, lambda o: a_copy((head + o) % heads, head).start())
    home[:, cols(head)] = a_send[rows(head), :]

    def forward(i):
        s = (p + n - i * plane) % n
        line_copy(i, s).wait_recv()
        over(plane, lambda o: plane_copy(i, o, s).start())

    over(lines, forward)

    over(heads, lambda o: a_copy((head + o) % heads, (head + heads - o) % heads).wait_recv())
    for load in late:
        load.wait()

    def p_copy(c):
        return pltpu.make_async_remote_copy(
            p_send.at[c], p_recv.at[c], p_ss.at[c], p_rs.at[c], device_id={"tp": 1 - t}
        )

    mine = []
    for c in range(chunks):
        part = jnp.dot(home[...], w[:, c * width : (c + 1) * width], preferred_element_type=F32)
        top, bottom = part[:half], part[half:]
        p_send[c] = jnp.where(t == 0, bottom, top).astype(BF16)
        p_copy(c).start()
        at = slice(c * width, (c + 1) * width)
        mine.append(jnp.where(t == 0, top, bottom))
    def finish_plane(o):
        def one(i, carry):
            s = i * plane + (p % plane + o) % plane
            plane_copy(None, o, s).wait_recv()
            return carry

        lax.fori_loop(0, lines, one, 0)
        plane_copy(None, o, p).wait_send()

    over(plane, finish_plane)
    stores = [
        pltpu.make_async_copy(src, dst, local_sem.at[11 + i])
        for i, (src, dst) in enumerate(((txt_out, txt_out_hbm), (out_ref, out_hbm)))
    ]
    stores[0].start()
    for c in range(chunks):
        at = slice(c * width, (c + 1) * width)
        p_copy(c).wait_recv()
        projected = mine[c] + p_recv[c].astype(F32)
        out_ref[:, at] = (
            res[:, at].astype(F32) + gate[:, at] * (projected + bias[:, at])
        ).astype(BF16)
    stores[1].start()

    def finish_line(i):
        s = (p + n - i * plane) % n
        over(plane, lambda o: plane_copy(i, o, s).wait_send())
        line_copy(i, s).wait_send()

    over(lines, finish_line)
    def finish_relay(relay):
        def one(o):
            def to_line(j, carry):
                relay(j, o, j * groups + group).wait_send()
                return carry

            lax.fori_loop(0, heads, to_line, 0)

        over(groups, one)

    finish_relay(k_relay)
    finish_relay(v_relay)
    over(heads, lambda o: k_copy((head + o) % heads, p).wait_send())
    over(heads, lambda o: v_copy((head + o) % heads, p).wait_send())
    over(heads, lambda o: q_copy((head + o) % heads, head).wait_send())
    over(heads, lambda o: a_copy((head + o) % heads, head).wait_send())
    for c in range(chunks):
        p_copy(c).wait_send()
    for copy in stores:
        copy.wait()


def shards(img_qkv, txt_qkv, frame_index, row_index, column_index, txt_len, residual, w_proj, proj_bias, gate):
    tokens = img_qkv.shape[1]
    channels = img_qkv.shape[3]
    heads = channels // HD
    n = lax.axis_size("seq")
    groups = n // heads
    text = txt_qkv.shape[1]
    share = text // groups
    plane = largest_divisor(n)
    lines = n // plane
    model = w_proj.shape[1]
    half = residual.shape[1]
    chunks = 4
    img = img_qkv[0].transpose(1, 0, 2)
    txt = txt_qkv[0].transpose(1, 0, 2)
    hbm = pl.BlockSpec(memory_space=pltpu.HBM)
    dma = pltpu.SemaphoreType.DMA
    out, txt_out = pl.pallas_call(
        functools.partial(kernel, n, heads),
        out_shape=(
            jax.ShapeDtypeStruct((half, model), BF16),
            jax.ShapeDtypeStruct((text, channels), BF16),
        ),
        in_specs=[hbm] * 5 + [pl.BlockSpec(memory_space=pltpu.SMEM)] + [hbm] * 4,
        out_specs=(hbm, hbm),
        scratch_shapes=[
            pltpu.VMEM((half, model), BF16),
            pltpu.VMEM((text, channels), BF16),
            pltpu.VMEM((3, tokens, channels), BF16),
            pltpu.VMEM((share, HD), BF16),
            pltpu.VMEM((3, 1, tokens), jnp.int32),
            pltpu.VMEM((heads, tokens, HD), BF16),
            pltpu.VMEM((heads, tokens, HD), BF16),
            pltpu.VMEM((heads * tokens, HD), BF16),
            pltpu.VMEM((n * tokens + text, HD), BF16),
            pltpu.VMEM((n * tokens + text, HD), BF16),
            pltpu.VMEM((heads * tokens, HD), BF16),
            pltpu.VMEM((tokens, channels), BF16),
            pltpu.VMEM((share, HD), BF16),
            pltpu.VMEM(w_proj.shape, BF16),
            pltpu.VMEM((half, model), BF16),
            pltpu.VMEM((1, model), F32),
            pltpu.VMEM((1, model), F32),
            pltpu.VMEM((chunks, half, model // chunks), BF16),
            pltpu.VMEM((chunks, half, model // chunks), BF16),
            dma((13,)),
            dma((heads,)), dma((heads,)),
            dma((heads,)), dma((n,)), dma((heads, groups)),
            dma((heads,)), dma((n,)), dma((heads, groups)),
            dma((heads,)), dma((heads,)),
            dma((lines,)), dma((lines, plane)), dma((n,)),
            dma((chunks,)), dma((chunks,)),
        ],
        compiler_params=pltpu.CompilerParams(
            collective_id=0, has_side_effects=True, vmem_limit_bytes=67043328
        ),
    )(
        img, txt, frame_index, row_index, column_index, txt_len, residual[0], w_proj,
        proj_bias[None], gate[None],
    )
    return out[None], txt_out[None]


def solution(mesh):
    in_specs = (
        P(None, "seq", None, "tp"),
        P(None, None, None, "tp"),
        P(None, "seq"),
        P(None, "seq"),
        P(None, "seq"),
        P(),
        P(None, ("seq", "tp"), None),
        P("tp", None),
        P(),
        P(),
    )
    out_specs = (P(None, ("seq", "tp"), None), P(None, None, "tp"))
    return jax.shard_map(shards, mesh=mesh, in_specs=in_specs, out_specs=out_specs, check_vma=False)
```
